32 devices in a mesh: grp: 2 (over y), seq: 8 (over z, x), head: 2 (over core).
Axes of the slice: x: 2, y: 2, z: 4, core: 2. Of those that a mesh axis runs over, the one named last changes fastest.
Arguments:
- queries: bfloat16 [6144, 768], P(('grp', 'seq'), 'head'), parts along dimension 0, may hold values from -6 to 6
- key_rows: bfloat16 [6144, 768], P(('grp', 'seq'), 'head'), parts along dimension 0, may hold values from -6 to 6
- value_rows: bfloat16 [6144, 768], P(('grp', 'seq'), 'head'), parts along dimension 0, may hold values from -6 to 6
- gate_input: bfloat16 [6144, 768], P(('grp', 'seq'), 'head'), parts along dimension 0, may hold values from -6 to 6
- norm_gain: float32 [768], P('head'), may hold values from 0.5 to 1.5
Outputs:
- retained: bfloat16 [6144, 768], P(('grp', 'seq'), 'head'), parts along dimension 0
- final_state: float32 [256, 6, 128], P(('grp', 'seq'), 'head'), parts along dimension 0
The draws below stay inside these ranges and needn't reach their ends.
There are 2 independent parts, one for each index of `grp`. The reference program is written for one: setup_inputs(seed, part) draws one part's arguments, and reference() takes and returns one part's arrays. A program takes and returns all parts, laid end to end along the dimension named above; an argument that names none is the same for every part. Nothing has to cross between parts.
All inputs are finite; a program needn't handle non-finite values.
Results may differ from the reference program's by a relative error of at most 0.0056.
Values sent between devices are 32-bit elements; how exact they have to be, the bound alone decides.
A program may use at most 128 MiB of HBM per device.

```python
import jax
import jax.numpy as jnp
from jax import lax

ALL_HEADS = 10
HEADS = 6
DH = 128
TOK_DEV = 384
LENGTH = 3072
N_SEQ = 8


def level_of(key, shape, shards, smallest, top_value):
    loudness, own = 1.0, jax.random.fold_in(key, 6)
    for position, blocks in shards:
        steps = jnp.exp(jax.random.uniform(jax.random.fold_in(own, position), (blocks,), jnp.float32, smallest / len(shards), top_value / len(shards)))
        loudness = loudness * jnp.repeat(steps, shape[position] // blocks).reshape([-1 if axis == position else 1 for axis in range(len(shape))])
    return loudness


def normal_values(key, dims, spread, most, pieces=(), kind=jnp.bfloat16):
    values = jax.random.normal(key, dims, jnp.float32) * spread
    if len(pieces) > 0:
        values = level_of(key, dims, pieces, -0.22, 0.18) * values
    return jnp.clip(values, min=-most, max=most).astype(kind)


def setup_inputs(seed: int = 0, part: int = 0) -> dict:
    key_of = jax.random.split(jax.random.key(seed), 6)
    part_splits = jax.random.split(jax.random.fold_in(key_of[5], part), 6)
    queries = normal_values(part_splits[0], (LENGTH, HEADS * DH), 1.0, 6.0, ((0, 8), (1, 2)))
    key_rows = normal_values(part_splits[1], (LENGTH, HEADS * DH), 1.0, 6.0, ((0, 8), (1, 2)))
    value_rows = normal_values(part_splits[2], (LENGTH, HEADS * DH), 1.0, 6.0, ((0, 8), (1, 2)))
    gate_input = normal_values(part_splits[3], (LENGTH, HEADS * DH), 1.0, 6.0, ((0, 8), (1, 2)))
    norm_gain = jnp.clip(1.0 + 0.1 * jax.random.normal(key_of[4], (HEADS * DH,), jnp.float32), 0.5, 1.5)
    return dict(queries=queries, key_rows=key_rows, value_rows=value_rows, gate_input=gate_input, norm_gain=norm_gain)


def reference(queries, key_rows, value_rows, gate_input, norm_gain):
    key_scale = DH ** (-0.5)
    head_ids = (ALL_HEADS - HEADS + jnp.arange(HEADS, dtype=jnp.int32)).astype(jnp.float32)
    log_decay = jnp.log1p(-jnp.exp2(-5.0 - head_ids))
    places = jnp.arange(TOK_DEV, dtype=jnp.float32)
    offsets = places[:, None] - places[None, :]
    causal = offsets >= 0
    decays = jnp.where(causal[None], jnp.exp(jnp.where(causal, offsets, 0.0)[None] * log_decay[:, None, None]), 0.0)
    tail_decay = jnp.exp((TOK_DEV - 1 - places)[:, None] * log_decay[None, :])
    lead_decay = jnp.exp((places + 1)[:, None] * log_decay[None, :])
    block_decay = jnp.exp(TOK_DEV * log_decay)
    gain_split = norm_gain.reshape(HEADS, DH)
    split_shape = (N_SEQ, TOK_DEV, HEADS, DH)
    highest = lax.Precision.HIGHEST

    def block_step(carried, block_data):
        query_split, key_split, value_split, gate_split = block_data
        query_wide = query_split.astype(jnp.float32)
        key_wide = key_split.astype(jnp.float32)
        value_wide = value_split.astype(jnp.float32)
        scores = jnp.einsum('thd,shd->hts', query_wide, key_wide, precision=highest) * key_scale
        weights = lax.optimization_barrier((scores * decays).astype(jnp.bfloat16)).astype(jnp.float32)
        inner_term = jnp.einsum('hts,shd->thd', weights, value_wide, precision=highest)
        keys_decayed = lax.optimization_barrier((key_wide * key_scale * tail_decay[:, :, None]).astype(jnp.bfloat16)).astype(jnp.float32)
        local_state = jnp.einsum('shi,shj->ihj', keys_decayed, value_wide, precision=highest)
        state_low = lax.optimization_barrier(carried.astype(jnp.bfloat16)).astype(jnp.float32)
        outer_term = jnp.einsum('thi,ihj->thj', query_wide, state_low, precision=highest) * lead_decay[:, :, None]
        mixture = inner_term + outer_term
        centred = mixture - lax.optimization_barrier(jnp.mean(mixture, axis=-1, keepdims=True))
        variance = lax.optimization_barrier(jnp.mean(centred * centred, axis=-1, keepdims=True))
        normed = centred * lax.rsqrt(variance + 1e-05) * gain_split
        result = (normed * jax.nn.silu(gate_split.astype(jnp.float32))).astype(jnp.bfloat16)
        updated = block_decay[None, :, None] * carried + local_state
        return (updated, result.reshape(TOK_DEV, HEADS * DH))
    initial = jnp.zeros((DH, HEADS, DH), jnp.float32)
    blocks = (queries.reshape(split_shape), key_rows.reshape(split_shape), value_rows.reshape(split_shape), gate_input.reshape(split_shape))
    final_state, outputs = lax.scan(block_step, initial, blocks)
    return (outputs.reshape(N_SEQ * TOK_DEV, HEADS * DH), final_state)
```

```python
import functools
import math

import jax
import jax.numpy as jnp
from jax import lax
from jax.experimental import pallas as pl
from jax.experimental.pallas import tpu as pltpu
from jax.sharding import PartitionSpec as P

ALL_HEADS = 10
HEADS = 6
DH = 128
MESH = pl.DeviceIdType.MESH
LOGS = [math.log1p(-(2.0 ** (-5 - (ALL_HEADS - HEADS + h)))) for h in range(HEADS)]


def flip(me, step, n):
    if n & (n - 1):
        return lax.rem(me + step, n)
    other = me
    bit = 1
    while bit < n:
        if step & bit:
            other = other + bit - 2 * bit * lax.rem(lax.div(me, bit), 2)
        bit *= 2
    return other


def each_peer(me, n, act):
    if n <= 16:
        for step in range(n - 1, 0, -1):
            act(flip(me, step, n))
    else:

        def go(step, carry):
            act(lax.rem(me + step, n))
            return carry

        lax.fori_loop(1, n, go, 0)


def kernel(
    n, heads, groups,
    q_hbm, k_hbm, v_hbm, g_hbm, gain_ref,
    out_ref, fin_ref,
    q, k, v, g, inner, gate, state, got, before, carried,
    load, send1, recv1, send2, recv2,
):
    me = lax.axis_index("seq")
    side = lax.axis_index("head")
    tokens = q.shape[0]
    rows = DH // n
    scale = DH ** (-0.5)

    loads = [
        pltpu.make_async_copy(src, dst, load.at[i])
        for i, (src, dst) in enumerate(((k_hbm, k), (v_hbm, v), (q_hbm, q), (g_hbm, g)))
    ]
    for copy in loads:
        copy.start()

    barrier = pltpu.get_barrier_semaphore()
    each_peer(
        me, n,
        lambda peer: pl.semaphore_signal(
            barrier, inc=1, device_id={"seq": peer}, device_id_type=MESH
        ),
    )

    logs = []
    for h in range(heads):
        log = jnp.float32(LOGS[h])
        for s in range(1, groups):
            log = jnp.where(side == s, jnp.float32(LOGS[s * heads + h]), log)
        logs.append(log)

    place = lax.broadcasted_iota(jnp.int32, (tokens, DH), 0).astype(jnp.float32)

    def cols(h):
        return slice(h * DH, (h + 1) * DH)

    def send(source, target, slot_of, sems, h):
        def act(peer):
            pltpu.make_async_remote_copy(
                src_ref=source.at[h, peer],
                dst_ref=target.at[h, me],
                send_sem=sems[0].at[h],
                recv_sem=sems[1].at[h],
                device_id={"seq": peer},
                device_id_type=MESH,
            ).start()

        each_peer(me, n, act)

    def drain(buffer, sem, h):
        piece = buffer.at[h, pl.ds(0, n - 1)]
        pltpu.make_async_copy(piece, piece, sem.at[h]).wait()

    loads[0].wait()
    loads[1].wait()
    for h in range(heads):
        tail = jnp.exp((tokens - 1 - place) * logs[h])
        kd = (k[:, cols(h)].astype(jnp.float32) * scale * tail).astype(jnp.bfloat16)
        local = lax.dot_general(
            kd, v[:, cols(h)], (((0,), (0,)), ((), ())), preferred_element_type=jnp.float32
        )
        state[h] = local.reshape(n, rows, DH)
    pl.semaphore_wait(barrier, n - 1)
    for h in range(heads):
        send(state, got, me, (send1, recv1), h)
        got[h, me] = state[h, me]

    loads[2].wait()
    offsets = (
        lax.broadcasted_iota(jnp.int32, (tokens, tokens), 0)
        - lax.broadcasted_iota(jnp.int32, (tokens, tokens), 1)
    ).astype(jnp.float32)
    causal = offsets >= 0
    for h in range(heads):
        scores = lax.dot_general(
            q[:, cols(h)], k[:, cols(h)], (((1,), (1,)), ((), ())),
            preferred_element_type=jnp.float32,
        ) * scale
        decays = jnp.where(causal, jnp.exp(jnp.where(causal, offsets, 0.0) * logs[h]), 0.0)
        weights = (scores * decays).astype(jnp.bfloat16)
        inner[h] = jnp.dot(weights, v[:, cols(h)], preferred_element_type=jnp.float32)
    loads[3].wait()
    for h in range(heads):
        u = g[:, cols(h)].astype(jnp.float32)
        gate[h] = u / (1.0 + jnp.exp(-u)) * gain_ref[:, cols(h)]

    for h in range(heads):
        drain(got, recv1, h)
        block_decay = jnp.exp(jnp.full((rows, DH), tokens, jnp.float32) * logs[h])

        def hop(b, total):
            before[h, b] = total
            return block_decay * total + got[h, b]

        total = jnp.zeros((rows, DH), jnp.float32)
        if n <= 16:
            for b in range(n):
                total = hop(b, total)
        else:
            total = lax.fori_loop(0, n, hop, total)
        send(before, carried, me, (send2, recv2), h)
        carried[h, me] = before[h, me]
        fin_ref[h] = total

    for h in range(heads):
        lead = jnp.exp((place + 1.0) * logs[h])
        drain(carried, recv2, h)
        low = carried[h].reshape(DH, DH).astype(jnp.bfloat16)
        outer = jnp.dot(q[:, cols(h)], low, preferred_element_type=jnp.float32)
        mixture = inner[h] + outer * lead
        centred = mixture - jnp.mean(mixture, axis=-1, keepdims=True)
        variance = jnp.mean(centred * centred, axis=-1, keepdims=True)
        normed = centred * lax.rsqrt(variance + 1e-05)
        out_ref[:, cols(h)] = (normed * gate[h]).astype(jnp.bfloat16)

    for h in range(heads):
        drain(state, send1, h)
        drain(before, send2, h)


def solution(mesh):
    n = mesh.shape["seq"]
    groups = mesh.shape["head"]

    def body(queries, key_rows, value_rows, gate_input, norm_gain):
        tokens, width = queries.shape
        heads = width // DH
        rows = DH // n
        slab = pltpu.VMEM((heads, n, rows, DH), jnp.float32)
        wide = pltpu.VMEM((tokens, width), jnp.bfloat16)
        tall = pltpu.VMEM((heads, tokens, DH), jnp.float32)
        anywhere = pl.BlockSpec(memory_space=pl.ANY)
        vmem = pl.BlockSpec(memory_space=pltpu.VMEM)
        retained, final = pl.pallas_call(
            functools.partial(kernel, n, heads, groups),
            out_shape=(
                jax.ShapeDtypeStruct((tokens, width), jnp.bfloat16),
                jax.ShapeDtypeStruct((heads, rows, DH), jnp.float32),
            ),
            in_specs=[anywhere] * 4 + [vmem],
            out_specs=(vmem, vmem),
            scratch_shapes=[wide] * 4 + [tall] * 2 + [slab] * 4
            + [pltpu.SemaphoreType.DMA((4,))] + [pltpu.SemaphoreType.DMA((heads,))] * 4,
            compiler_params=pltpu.CompilerParams(collective_id=0, has_side_effects=True),
            name="retention",
        )(queries, key_rows, value_rows, gate_input, norm_gain.reshape(1, width))
        return retained, final.transpose(1, 0, 2)

    return jax.shard_map(
        body,
        mesh=mesh,
        in_specs=(P(("grp", "seq"), "head"),) * 4 + (P("head"),),
        out_specs=(P(("grp", "seq"), "head"), P(("grp", "seq"), "head", None)),
        check_vma=False,
    )
```

```python
import functools
import math

import jax
import jax.numpy as jnp
from jax import lax
from jax.experimental import pallas as pl
from jax.experimental.pallas import tpu as pltpu
from jax.sharding import PartitionSpec as P

ALL_HEADS = 10
HEADS = 6
DH = 128
MESH = pl.DeviceIdType.MESH
LOGS = [math.log1p(-(2.0 ** (-5 - (ALL_HEADS - HEADS + h)))) for h in range(HEADS)]


def flip(me, step, n):
    if n & (n - 1):
        return lax.rem(me + step, n)
    other = me
    bit = 1
    while bit < n:
        if step & bit:
            other = other + bit - 2 * bit * lax.rem(lax.div(me, bit), 2)
        bit *= 2
    return other


def each_peer(me, n, act):
    if n <= 16:
        for step in range(n - 1, 0, -1):
            act(flip(me, step, n))
    else:

        def go(step, carry):
            act(lax.rem(me + step, n))
            return carry

        lax.fori_loop(1, n, go, 0)


def kernel(
    n, heads, groups,
    q_hbm, k_hbm, v_hbm, g_hbm, gain_ref,
    out_ref, fin_ref,
    q, k, v, g, inner, gate, state, got, before, carried,
    load, send1, recv1, send2, recv2,
):
    me = lax.axis_index("seq")
    side = lax.axis_index("head")
    tokens = q.shape[0]
    rows = DH // n
    scale = DH ** (-0.5)

    loads = [
        pltpu.make_async_copy(src, dst, load.at[i])
        for i, (src, dst) in enumerate(((k_hbm, k), (v_hbm, v), (q_hbm, q), (g_hbm, g)))
    ]
    for copy in loads:
        copy.start()

    barrier = pltpu.get_barrier_semaphore()
    each_peer(
        me, n,
        lambda peer: pl.semaphore_signal(
            barrier, inc=1, device_id={"seq": peer}, device_id_type=MESH
        ),
    )

    logs = []
    for h in range(heads):
        log = jnp.float32(LOGS[h])
        for s in range(1, groups):
            log = jnp.where(side == s, jnp.float32(LOGS[s * heads + h]), log)
        logs.append(log)

    place = lax.broadcasted_iota(jnp.int32, (tokens, DH), 0).astype(jnp.float32)

    def cols(h):
        return slice(h * DH, (h + 1) * DH)

    def send(source, target, slot_of, sems, h):
        def act(peer):
            pltpu.make_async_remote_copy(
                src_ref=source.at[h, peer],
                dst_ref=target.at[h, me],
                send_sem=sems[0].at[h],
                recv_sem=sems[1].at[h],
                device_id={"seq": peer},
                device_id_type=MESH,
            ).start()

        each_peer(me, n, act)

    def drain(buffer, sem, h):
        piece = buffer.at[h, pl.ds(0, n - 1)]
        pltpu.make_async_copy(piece, piece, sem.at[h]).wait()

    loads[0].wait()
    loads[1].wait()
    for h in range(heads):
        tail = jnp.exp((tokens - 1 - place) * logs[h])
        kd = (k[:, cols(h)].astype(jnp.float32) * scale * tail).astype(jnp.bfloat16)
        local = lax.dot_general(
            kd, v[:, cols(h)], (((0,), (0,)), ((), ())), preferred_element_type=jnp.float32
        )
        state[h] = local.reshape(n, rows, DH)
        if h == 0:
            pl.semaphore_wait(barrier, n - 1)
        send(state, got, me, (send1, recv1), h)
        got[h, me] = state[h, me]

    loads[2].wait()
    offsets = (
        lax.broadcasted_iota(jnp.int32, (tokens, tokens), 0)
        - lax.broadcasted_iota(jnp.int32, (tokens, tokens), 1)
    ).astype(jnp.float32)
    causal = offsets >= 0
    for h in range(heads):
        scores = lax.dot_general(
            q[:, cols(h)], k[:, cols(h)], (((1,), (1,)), ((), ())),
            preferred_element_type=jnp.float32,
        ) * scale
        decays = jnp.where(causal, jnp.exp(jnp.where(causal, offsets, 0.0) * logs[h]), 0.0)
        weights = (scores * decays).astype(jnp.bfloat16)
        inner[h] = jnp.dot(weights, v[:, cols(h)], preferred_element_type=jnp.float32)
    loads[3].wait()
    for h in range(heads):
        u = g[:, cols(h)].astype(jnp.float32)
        gate[h] = u / (1.0 + jnp.exp(-u)) * gain_ref[cols(h)][None, :]

    for h in range(heads):
        drain(got, recv1, h)
        block_decay = jnp.exp(jnp.full((rows, DH), tokens, jnp.float32) * logs[h])

        def hop(b, total):
            before[h, b] = total
            return block_decay * total + got[h, b]

        total = jnp.zeros((rows, DH), jnp.float32)
        if n <= 16:
            for b in range(n):
                total = hop(b, total)
        else:
            total = lax.fori_loop(0, n, hop, total)
        send(before, carried, me, (send2, recv2), h)
        carried[h, me] = before[h, me]
        fin_ref[h] = total

    for h in range(heads):
        lead = jnp.exp((place + 1.0) * logs[h])
        drain(carried, recv2, h)
        low = carried[h].reshape(DH, DH).astype(jnp.bfloat16)
        outer = jnp.dot(q[:, cols(h)], low, preferred_element_type=jnp.float32)
        mixture = inner[h] + outer * lead
        centred = mixture - jnp.mean(mixture, axis=-1, keepdims=True)
        variance = jnp.mean(centred * centred, axis=-1, keepdims=True)
        normed = centred * lax.rsqrt(variance + 1e-05)
        out_ref[:, cols(h)] = (normed * gate[h]).astype(jnp.bfloat16)

    for h in range(heads):
        drain(state, send1, h)
        drain(before, send2, h)


def solution(mesh):
    n = mesh.shape["seq"]
    groups = mesh.shape["head"]

    def body(queries, key_rows, value_rows, gate_input, norm_gain):
        tokens, width = queries.shape
        heads = width // DH
        rows = DH // n
        slab = pltpu.VMEM((heads, n, rows, DH), jnp.float32)
        wide = pltpu.VMEM((tokens, width), jnp.bfloat16)
        tall = pltpu.VMEM((heads, tokens, DH), jnp.float32)
        anywhere = pl.BlockSpec(memory_space=pltpu.HBM)
        vmem = pl.BlockSpec(memory_space=pltpu.VMEM)
        retained, final = pl.pallas_call(
            functools.partial(kernel, n, heads, groups),
            out_shape=(
                pltpu.VMEM((tokens, width), jnp.bfloat16),
                pltpu.VMEM((heads, rows, DH), jnp.float32),
            ),
            in_specs=[anywhere] * 4 + [vmem],
            out_specs=(vmem, vmem),
            scratch_shapes=[wide] * 4 + [tall] * 2 + [slab] * 4
            + [pltpu.SemaphoreType.DMA((4,))] + [pltpu.SemaphoreType.DMA((heads,))] * 4,
            compiler_params=pltpu.CompilerParams(collective_id=0, has_side_effects=True),
            name="retention",
        )(queries, key_rows, value_rows, gate_input, norm_gain)
        return retained, final.transpose(1, 0, 2)

    return jax.shard_map(
        body,
        mesh=mesh,
        in_specs=(P(("grp", "seq"), "head"),) * 4 + (P("head"),),
        out_specs=(P(("grp", "seq"), "head"), P(("grp", "seq"), "head", None)),
        check_vma=False,
    )
```

```python
import functools
import math

import jax
import jax.numpy as jnp
from jax import lax
from jax.experimental import pallas as pl
from jax.experimental.pallas import tpu as pltpu
from jax.sharding import PartitionSpec as P

ALL_HEADS = 10
HEADS = 6
DH = 128
MESH = pl.DeviceIdType.MESH
LOGS = [math.log1p(-(2.0 ** (-5 - (ALL_HEADS - HEADS + h)))) for h in range(HEADS)]


def flip(me, step, n):
    if n & (n - 1):
        return lax.rem(me + step, n)
    other = me
    bit = 1
    while bit < n:
        if step & bit:
            other = other + bit - 2 * bit * lax.rem(lax.div(me, bit), 2)
        bit *= 2
    return other


def each_peer(me, n, act):
    if n <= 16:
        for step in range(n - 1, 0, -1):
            act(flip(me, step, n))
    else:

        def go(step, carry):
            act(lax.rem(me + step, n))
            return carry

        lax.fori_loop(1, n, go, 0)


def kernel(
    n, heads, groups,
    q_hbm, k_hbm, v_hbm, g_hbm, gain_ref,
    out_ref, fin_ref,
    q, k, v, g, inner, gate, state, got, before, carried,
    load, send1, recv1, send2, recv2,
):
    me = lax.axis_index("seq")
    side = lax.axis_index("head")
    tokens = q.shape[0]
    rows = DH // n
    scale = DH ** (-0.5)

    loads = [
        pltpu.make_async_copy(src, dst, load.at[i])
        for i, (src, dst) in enumerate(((k_hbm, k), (v_hbm, v), (q_hbm, q), (g_hbm, g)))
    ]
    for copy in loads:
        copy.start()

    barrier = pltpu.get_barrier_semaphore()
    each_peer(
        me, n,
        lambda peer: pl.semaphore_signal(
            barrier, inc=1, device_id={"seq": peer}, device_id_type=MESH
        ),
    )

    logs = []
    for h in range(heads):
        log = jnp.float32(LOGS[h])
        for s in range(1, groups):
            log = jnp.where(side == s, jnp.float32(LOGS[s * heads + h]), log)
        logs.append(log)

    place = lax.broadcasted_iota(jnp.int32, (tokens, DH), 0).astype(jnp.float32)

    def cols(h):
        return slice(h * DH, (h + 1) * DH)

    def send(source, target, slot_of, sems, h):
        def act(peer):
            pltpu.make_async_remote_copy(
                src_ref=source.at[h, peer],
                dst_ref=target.at[h, me],
                send_sem=sems[0].at[h],
                recv_sem=sems[1].at[h],
                device_id={"seq": peer},
                device_id_type=MESH,
            ).start()

        each_peer(me, n, act)

    def drain(buffer, sem, h):
        piece = buffer.at[h, pl.ds(0, n - 1)]
        pltpu.make_async_copy(piece, piece, sem.at[h]).wait()

    loads[0].wait()
    loads[1].wait()
    for h in range(heads):
        tail = jnp.exp((tokens - 1 - place) * logs[h])
        kd = (k[:, cols(h)].astype(jnp.float32) * scale * tail).astype(jnp.bfloat16)
        local = lax.dot_general(
            kd, v[:, cols(h)], (((0,), (0,)), ((), ())), preferred_element_type=jnp.float32
        )
        state[h] = local.reshape(n, rows, DH)
        if h == 0:
            pl.semaphore_wait(barrier, n - 1)
        send(state, got, me, (send1, recv1), h)
        got[h, me] = state[h, me]

    loads[2].wait()
    offsets = (
        lax.broadcasted_iota(jnp.int32, (tokens, tokens), 0)
        - lax.broadcasted_iota(jnp.int32, (tokens, tokens), 1)
    ).astype(jnp.float32)
    causal = offsets >= 0
    for h in range(heads):
        scores = lax.dot_general(
            q[:, cols(h)], k[:, cols(h)], (((1,), (1,)), ((), ())),
            preferred_element_type=jnp.float32,
        ) * scale
        decays = jnp.where(causal, jnp.exp(jnp.where(causal, offsets, 0.0) * logs[h]), 0.0)
        weights = (scores * decays).astype(jnp.bfloat16)
        inner[h] = jnp.dot(weights, v[:, cols(h)], preferred_element_type=jnp.float32)
    loads[3].wait()
    for h in range(heads):
        u = g[:, cols(h)].astype(jnp.float32)
        gate[h] = u / (1.0 + jnp.exp(-u)) * gain_ref[cols(h)][None, :]

    for h in range(heads):
        drain(got, recv1, h)
        block_decay = jnp.exp(jnp.full((rows, DH), tokens, jnp.float32) * logs[h])

        def hop(b, total):
            before[h, b] = total
            return block_decay * total + got[h, b]

        total = jnp.zeros((rows, DH), jnp.float32)
        if n <= 16:
            for b in range(n):
                total = hop(b, total)
        else:
            total = lax.fori_loop(0, n, hop, total)
        send(before, carried, me, (send2, recv2), h)
        carried[h, me] = before[h, me]
        fin_ref[h] = total

    for h in range(heads):
        lead = jnp.exp((place + 1.0) * logs[h])
        drain(carried, recv2, h)
        low = carried[h].reshape(DH, DH).astype(jnp.bfloat16)
        outer = jnp.dot(q[:, cols(h)], low, preferred_element_type=jnp.float32)
        mixture = inner[h] + outer * lead
        centred = mixture - jnp.mean(mixture, axis=-1, keepdims=True)
        variance = jnp.mean(centred * centred, axis=-1, keepdims=True)
        normed = centred * lax.rsqrt(variance + 1e-05)
        out_ref[:, cols(h)] = (normed * gate[h]).astype(jnp.bfloat16)

    for h in range(heads):
        drain(state, send1, h)
        drain(before, send2, h)


def settle(res, fin, out_hbm, fin_hbm, sems):
    copies = [
        pltpu.make_async_copy(res, out_hbm, sems.at[0]),
        pltpu.make_async_copy(fin, fin_hbm, sems.at[1]),
    ]
    for copy in copies:
        copy.start()
    for copy in copies:
        copy.wait()


def solution(mesh):
    n = mesh.shape["seq"]
    groups = mesh.shape["head"]

    def body(queries, key_rows, value_rows, gate_input, norm_gain):
        tokens, width = queries.shape
        heads = width // DH
        rows = DH // n
        slab = pltpu.VMEM((heads, n, rows, DH), jnp.float32)
        wide = pltpu.VMEM((tokens, width), jnp.bfloat16)
        tall = pltpu.VMEM((heads, tokens, DH), jnp.float32)
        anywhere = pl.BlockSpec(memory_space=pltpu.HBM)
        vmem = pl.BlockSpec(memory_space=pltpu.VMEM)
        retained, final = pl.pallas_call(
            functools.partial(kernel, n, heads, groups),
            out_shape=(
                pltpu.VMEM((tokens, width), jnp.bfloat16),
                pltpu.VMEM((heads, rows, DH), jnp.float32),
            ),
            in_specs=[anywhere] * 4 + [vmem],
            out_specs=(vmem, vmem),
            scratch_shapes=[wide] * 4 + [tall] * 2 + [slab] * 4
            + [pltpu.SemaphoreType.DMA((4,))] + [pltpu.SemaphoreType.DMA((heads,))] * 4,
            compiler_params=pltpu.CompilerParams(collective_id=0, has_side_effects=True),
            name="retention",
        )(queries, key_rows, value_rows, gate_input, norm_gain)
        retained, final = pl.pallas_call(
            settle,
            out_shape=(
                jax.ShapeDtypeStruct((tokens, width), jnp.bfloat16),
                jax.ShapeDtypeStruct((heads, rows, DH), jnp.float32),
            ),
            in_specs=[vmem] * 2,
            out_specs=(anywhere, anywhere),
            scratch_shapes=[pltpu.SemaphoreType.DMA((2,))],
            compiler_params=pltpu.CompilerParams(vmem_limit_bytes=1 << 20, has_side_effects=True),
            name="settle",
        )(retained, final)
        return retained, final.transpose(1, 0, 2)

    return jax.shard_map(
        body,
        mesh=mesh,
        in_specs=(P(("grp", "seq"), "head"),) * 4 + (P("head"),),
        out_specs=(P(("grp", "seq"), "head"), P(("grp", "seq"), "head", None)),
        check_vma=False,
    )
```

```python
import functools
import math

import jax
import jax.numpy as jnp
from jax import lax
from jax.experimental import pallas as pl
from jax.experimental.pallas import tpu as pltpu
from jax.sharding import PartitionSpec as P

ALL_HEADS = 10
HEADS = 6
DH = 128
MESH = pl.DeviceIdType.MESH
LOGS = [math.log1p(-(2.0 ** (-5 - (ALL_HEADS - HEADS + h)))) for h in range(HEADS)]


def flip(me, step, n):
    if n & (n - 1):
        return lax.rem(me + step, n)
    other = me
    bit = 1
    while bit < n:
        if step & bit:
            other = other + bit - 2 * bit * lax.rem(lax.div(me, bit), 2)
        bit *= 2
    return other


def each_peer(me, n, act):
    if n <= 16:
        for step in range(n - 1, 0, -1):
            act(flip(me, step, n))
    else:

        def go(step, carry):
            act(lax.rem(me + step, n))
            return carry

        lax.fori_loop(1, n, go, 0)


def kernel(
    n, heads, groups,
    q_hbm, k_hbm, v_hbm, g_hbm, gain_ref,
    out_ref, fin_ref,
    q, k, v, g, inner, gate, state, got, before, carried,
    load, send1, recv1, send2, recv2,
):
    me = lax.axis_index("seq")
    side = lax.axis_index("head")
    tokens = q.shape[0]
    rows = DH // n
    scale = DH ** (-0.5)

    loads = [
        pltpu.make_async_copy(src, dst, load.at[i])
        for i, (src, dst) in enumerate(((k_hbm, k), (v_hbm, v), (q_hbm, q), (g_hbm, g)))
    ]
    for copy in loads:
        copy.start()

    barrier = pltpu.get_barrier_semaphore()
    each_peer(
        me, n,
        lambda peer: pl.semaphore_signal(
            barrier, inc=1, device_id={"seq": peer}, device_id_type=MESH
        ),
    )

    logs = []
    for h in range(heads):
        log = jnp.float32(LOGS[h])
        for s in range(1, groups):
            log = jnp.where(side == s, jnp.float32(LOGS[s * heads + h]), log)
        logs.append(log)

    place = lax.broadcasted_iota(jnp.int32, (tokens, DH), 0).astype(jnp.float32)

    def cols(h):
        return slice(h * DH, (h + 1) * DH)

    def send(source, target, sems):
        def act(peer):
            pltpu.make_async_remote_copy(
                src_ref=source.at[peer],
                dst_ref=target.at[me],
                send_sem=sems[0].at[0],
                recv_sem=sems[1].at[0],
                device_id={"seq": peer},
                device_id_type=MESH,
            ).start()

        each_peer(me, n, act)

    def drain(buffer, sem, h):
        piece = buffer.at[pl.ds(0, n - 1)]
        pltpu.make_async_copy(piece, piece, sem.at[0]).wait()

    loads[0].wait()
    loads[1].wait()
    for h in range(heads):
        tail = jnp.exp((tokens - 1 - place) * logs[h])
        kd = (k[:, cols(h)].astype(jnp.float32) * scale * tail).astype(jnp.bfloat16)
        local = lax.dot_general(
            kd, v[:, cols(h)], (((0,), (0,)), ((), ())), preferred_element_type=jnp.float32
        )
        state[:, h] = local.reshape(n, rows, DH)
        if h == 0:
            pl.semaphore_wait(barrier, n - 1)
        if h == heads - 1:
            send(state, got, (send1, recv1))
            got[me] = state[me]

    loads[2].wait()
    offsets = (
        lax.broadcasted_iota(jnp.int32, (tokens, tokens), 0)
        - lax.broadcasted_iota(jnp.int32, (tokens, tokens), 1)
    ).astype(jnp.float32)
    causal = offsets >= 0
    for h in range(heads):
        scores = lax.dot_general(
            q[:, cols(h)], k[:, cols(h)], (((1,), (1,)), ((), ())),
            preferred_element_type=jnp.float32,
        ) * scale
        decays = jnp.where(causal, jnp.exp(jnp.where(causal, offsets, 0.0) * logs[h]), 0.0)
        weights = (scores * decays).astype(jnp.bfloat16)
        inner[h] = jnp.dot(weights, v[:, cols(h)], preferred_element_type=jnp.float32)
    loads[3].wait()
    for h in range(heads):
        u = g[:, cols(h)].astype(jnp.float32)
        gate[h] = u / (1.0 + jnp.exp(-u)) * gain_ref[cols(h)][None, :]

    for h in range(heads):
        if h == 0:
            drain(got, recv1, h)
        block_decay = jnp.exp(jnp.full((rows, DH), tokens, jnp.float32) * logs[h])

        def hop(b, total):
            before[b, h] = total
            return block_decay * total + got[b, h]

        total = jnp.zeros((rows, DH), jnp.float32)
        if n <= 16:
            for b in range(n):
                total = hop(b, total)
        else:
            total = lax.fori_loop(0, n, hop, total)
        if h == heads - 1:
            send(before, carried, (send2, recv2))
            carried[me] = before[me]
        fin_ref[h] = total

    for h in range(heads):
        lead = jnp.exp((place + 1.0) * logs[h])
        if h == 0:
            drain(carried, recv2, h)
        low = carried[:, h].reshape(DH, DH).astype(jnp.bfloat16)
        outer = jnp.dot(q[:, cols(h)], low, preferred_element_type=jnp.float32)
        mixture = inner[h] + outer * lead
        centred = mixture - jnp.mean(mixture, axis=-1, keepdims=True)
        variance = jnp.mean(centred * centred, axis=-1, keepdims=True)
        normed = centred * lax.rsqrt(variance + 1e-05)
        out_ref[:, cols(h)] = (normed * gate[h]).astype(jnp.bfloat16)

    drain(state, send1, 0)
    drain(before, send2, 0)


def settle(res, fin, out_hbm, fin_hbm, sems):
    copies = [
        pltpu.make_async_copy(res, out_hbm, sems.at[0]),
        pltpu.make_async_copy(fin, fin_hbm, sems.at[1]),
    ]
    for copy in copies:
        copy.start()
    for copy in copies:
        copy.wait()


def solution(mesh):
    n = mesh.shape["seq"]
    groups = mesh.shape["head"]

    def body(queries, key_rows, value_rows, gate_input, norm_gain):
        tokens, width = queries.shape
        heads = width // DH
        rows = DH // n
        slab = pltpu.VMEM((n, heads, rows, DH), jnp.float32)
        wide = pltpu.VMEM((tokens, width), jnp.bfloat16)
        tall = pltpu.VMEM((heads, tokens, DH), jnp.float32)
        anywhere = pl.BlockSpec(memory_space=pltpu.HBM)
        vmem = pl.BlockSpec(memory_space=pltpu.VMEM)
        retained, final = pl.pallas_call(
            functools.partial(kernel, n, heads, groups),
            out_shape=(
                pltpu.VMEM((tokens, width), jnp.bfloat16),
                pltpu.VMEM((heads, rows, DH), jnp.float32),
            ),
            in_specs=[anywhere] * 4 + [vmem],
            out_specs=(vmem, vmem),
            scratch_shapes=[wide] * 4 + [tall] * 2 + [slab] * 4
            + [pltpu.SemaphoreType.DMA((4,))] + [pltpu.SemaphoreType.DMA((heads,))] * 4,
            compiler_params=pltpu.CompilerParams(collective_id=0, has_side_effects=True),
            name="retention",
        )(queries, key_rows, value_rows, gate_input, norm_gain)
        retained, final = pl.pallas_call(
            settle,
            out_shape=(
                jax.ShapeDtypeStruct((tokens, width), jnp.bfloat16),
                jax.ShapeDtypeStruct((heads, rows, DH), jnp.float32),
            ),
            in_specs=[vmem] * 2,
            out_specs=(anywhere, anywhere),
            scratch_shapes=[pltpu.SemaphoreType.DMA((2,))],
            compiler_params=pltpu.CompilerParams(vmem_limit_bytes=1 << 20, has_side_effects=True),
            name="settle",
        )(retained, final)
        return retained, final.transpose(1, 0, 2)

    return jax.shard_map(
        body,
        mesh=mesh,
        in_specs=(P(("grp", "seq"), "head"),) * 4 + (P("head"),),
        out_specs=(P(("grp", "seq"), "head"), P(("grp", "seq"), "head", None)),
        check_vma=False,
    )
```
